32 devices in a mesh: dp: 4 (over y, x), expert: 8 (over z, core).
Axes of the slice: x: 2, y: 2, z: 4, core: 2. Of those that a mesh axis runs over, the one named last changes fastest.
Arguments:
- tokens: bfloat16 [4096, 4096], P(('dp', 'expert')), may hold values from -6 to 6
- gate_proj: bfloat16 [8, 768, 4096], P('expert', 'dp'), may hold values from -0.09375 to 0.09375
- up_proj: bfloat16 [8, 768, 4096], P('expert', 'dp'), may hold values from -0.09375 to 0.09375
- down_proj: bfloat16 [8, 768, 4096], P('expert', 'dp'), may hold values from -0.21875 to 0.21875
- route_ids: int32 [4096, 2], P(('dp', 'expert')), may hold values from 0 to 7, as said below
- route_slots: int32 [4096, 2], P(('dp', 'expert')), may hold values from 0 to 95, as said below
- route_gates: float32 [4096, 2], P(('dp', 'expert')), may hold values from 0.1 to 1
- image_shard: int32 [4, 8], P(None, 'expert'), may hold values from 0 to 3, as said below
- norm_gain: float32 [4096], replicated, may hold values from 0.5 to 1.5
- key_proj: bfloat16 [4096, 1024], P('dp'), may hold values from -0.09375 to 0.09375
Outputs:
- student_rows: bfloat16 [4096, 4096], P(('dp', 'expert'))
- keys: bfloat16 [4096, 1024], P(('dp', 'expert'))
The draws below stay inside these ranges and needn't reach their ends.
Inputs may be any that keep to these rules, and one draw needn't show every extreme that they name: `route_ids`: within the rows of one device a token names 2 different experts and no expert is named more than 2 * 48 times; on every device some expert is named exactly 2 * 48 times. `route_slots`: within the rows of one device the mentions of one expert carry the numbers 0 up to their count minus one, each once; one expert has 48 retained mentions from every device. `image_shard`: for each e, of the 4 image tiles of column e exactly 1 name each shard.
All inputs are finite; a program needn't handle non-finite values.
Results may differ from the reference program's by a relative error of at most 0.007.
Values may be sent and summed in bfloat16 or wider, within the bound.
A program may use at most 128 MiB of HBM per device.

```python
import math
import jax
import jax.numpy as jnp
from jax import lax

D = 4096
EFF = 768
KV_WIDTH = 1024
TOPK = 2
IMG_TOK = 128
TOK_DEV = 128
EXPERTS = 8
CAP = 48
IMG_DEV = 1
TOKENS = 4096
N_DP = 4
N_EXPERT = 8


def route_table(key):
    block_count = TOKENS // TOK_DEV
    queue_depth = 2 * CAP
    cell_count = EXPERTS * queue_depth
    tickets = TOK_DEV * TOPK
    liking = 1 + jax.random.randint(jax.random.fold_in(key, 11), (EXPERTS, 1), 0, 4)
    favored = jax.random.randint(jax.random.fold_in(key, 12), (), 0, EXPERTS)
    expert_of = jnp.arange(cell_count, dtype=jnp.int32) // queue_depth

    def one_block(position):
        block_key = jax.random.fold_in(jax.random.fold_in(key, 13), position)
        busiest = jax.random.randint(jax.random.fold_in(block_key, 1), (), 0, EXPERTS)
        base_score = jax.random.randint(jax.random.fold_in(block_key, 2), (EXPERTS, queue_depth), 0, 65536)
        base_score = (base_score * liking).reshape(-1)
        forced = (expert_of == favored) | (expert_of == busiest)
        ranking = jnp.where(forced, 262144, base_score) * cell_count + jnp.arange(cell_count, dtype=jnp.int32)
        chosen = jnp.sort(lax.top_k(ranking, tickets)[1].astype(jnp.int32))
        chosen_experts = chosen // queue_depth
        before = jnp.sum((chosen_experts[None, :] < chosen_experts[:, None]).astype(jnp.int32), axis=1)
        queue_slots = jnp.arange(tickets, dtype=jnp.int32) - before
        layout_ids = chosen_experts.reshape(TOPK, TOK_DEV).T
        layout_slots = queue_slots.reshape(TOPK, TOK_DEV).T
        shuffle = jax.random.permutation(jax.random.fold_in(block_key, 3), TOK_DEV)
        return (layout_ids[shuffle], layout_slots[shuffle])
    all_ids, all_slots = jax.vmap(one_block)(jnp.arange(block_count, dtype=jnp.int32))
    return (all_ids.reshape(TOKENS, TOPK).astype(jnp.int32), all_slots.reshape(TOKENS, TOPK).astype(jnp.int32))


def draw_route_ids(key, part):
    return route_table(key)[0]


def draw_route_slots(key, part):
    return route_table(key)[1]


def draw_image_shard(key, part):
    images_col = N_DP * IMG_DEV

    def column(position):
        column_key = jax.random.fold_in(jax.random.fold_in(key, 21), position)
        return jax.random.permutation(column_key, images_col).astype(jnp.int32) // IMG_DEV
    layout = jax.vmap(column)(jnp.arange(N_EXPERT, dtype=jnp.int32))
    return layout.reshape(N_EXPERT, N_DP, IMG_DEV).transpose(1, 0, 2).reshape(N_DP, N_EXPERT * IMG_DEV)


def block_levels(own_key, extent, split, smallest, high):
    gain, own = 1.0, jax.random.fold_in(own_key, 6)
    for dim, blocks in split:
        heights = jnp.exp(jax.random.uniform(jax.random.fold_in(own, dim), (blocks,), jnp.float32, smallest / len(split), high / len(split)))
        gain = gain * jnp.repeat(heights, extent[dim] // blocks).reshape([-1 if axis == dim else 1 for axis in range(len(extent))])
    return gain


def centred(stream_key, shape, deviation, reach, pieces=(), held_as=jnp.bfloat16):
    entries = deviation * jax.random.normal(stream_key, shape, jnp.float32)
    if pieces:
        entries = entries * block_levels(stream_key, shape, pieces, -0.22, 0.18)
    return jnp.clip(entries, -reach, reach).astype(held_as)


def setup_inputs(seed: int = 0) -> dict:
    streams_of = jax.random.split(jax.random.key(seed), 11)
    return {
        "tokens": centred(streams_of[0], (TOKENS, D), 1.0, 6.0, ((0, 32),)),
        "gate_proj": centred(streams_of[1], (EXPERTS, EFF, D), D ** -0.5, 0.09375, ((0, 8), (1, 4))),
        "up_proj": centred(streams_of[2], (EXPERTS, EFF, D), D ** -0.5, 0.09375, ((0, 8), (1, 4))),
        "down_proj": centred(streams_of[3], (EXPERTS, EFF, D), EFF ** -0.5, 0.21875, ((0, 8), (1, 4))),
        "route_ids": draw_route_ids(jax.random.fold_in(streams_of[10], 71), 0),
        "route_slots": draw_route_slots(jax.random.fold_in(streams_of[10], 71), 0),
        "route_gates": jnp.clip(jnp.exp(math.log(1.0) - 2.3025851 * jax.random.uniform(streams_of[6], (TOKENS, TOPK), jnp.float32) ** block_levels(streams_of[6], (TOKENS, TOPK), ((0, 32),), -0.2, 0.2)), 0.1, 1.0),
        "image_shard": draw_image_shard(jax.random.fold_in(streams_of[10], 71), 0),
        "norm_gain": jnp.clip(1.0 + 0.1 * jax.random.normal(streams_of[8], (D,), jnp.float32), 0.5, 1.5),
        "key_proj": centred(streams_of[9], (D, KV_WIDTH), D ** -0.5, 0.09375, ((0, 4),)),
    }


def normalize(values, norm_gain):
    wide = values.astype(jnp.float32)
    mean_square = lax.optimization_barrier(jnp.mean(wide * wide, axis=-1, keepdims=True))
    return (wide * lax.rsqrt(mean_square + 1e-05) * norm_gain).astype(jnp.bfloat16)

def reference(tokens, gate_proj, up_proj, down_proj, route_ids, route_slots, route_gates, image_shard, norm_gain, key_proj):
    block_count = N_DP * N_EXPERT
    slot_total = EXPERTS * CAP
    blocks = tokens.reshape(block_count, TOK_DEV, D)
    choice_ids = route_ids.reshape(block_count, TOK_DEV * TOPK)
    choice_slots = route_slots.reshape(block_count, TOK_DEV * TOPK)
    choice_gates = route_gates.reshape(block_count, TOK_DEV * TOPK)
    retained = choice_slots < CAP
    slot_cells = jnp.where(retained, choice_ids * CAP + choice_slots, slot_total).astype(jnp.int32)
    owners = jnp.arange(TOK_DEV * TOPK, dtype=jnp.int32) // TOPK

    def fill_tokens(cell_row):
        return jnp.full((slot_total + 1,), TOK_DEV, jnp.int32).at[cell_row].set(owners)[:slot_total]

    def fill_gates(cell_row, gate_row):
        return jnp.zeros((slot_total + 1,), jnp.float32).at[cell_row].set(gate_row.astype(jnp.float32))[:slot_total]
    cell_token = jax.vmap(fill_tokens)(slot_cells).reshape(block_count, EXPERTS, CAP)
    cell_gate = jax.vmap(fill_gates)(slot_cells, choice_gates).reshape(block_count, EXPERTS, CAP)

    def take_rows(block, senders):
        return jnp.take(block, senders, axis=0, mode='fill', fill_value=0)

    def add_rows(running, senders, contribution):
        return running.at[senders].add(contribution, mode='drop')

    def expert_step(accumulated, expert):
        senders = lax.dynamic_index_in_dim(cell_token, expert, 1, keepdims=False)
        weights_now = lax.dynamic_index_in_dim(cell_gate, expert, 1, keepdims=False)
        gathered = jax.vmap(take_rows)(blocks, senders).reshape(block_count * CAP, D)
        gate_rows = lax.dynamic_index_in_dim(gate_proj, expert, 0, keepdims=False)
        up_rows = lax.dynamic_index_in_dim(up_proj, expert, 0, keepdims=False)
        down_rows = lax.dynamic_index_in_dim(down_proj, expert, 0, keepdims=False)
        dims = (((1,), (1,)), ((), ()))
        gate_act = lax.dot_general(gathered, gate_rows, dims, preferred_element_type=jnp.float32)
        up_act = lax.dot_general(gathered, up_rows, dims, preferred_element_type=jnp.float32)
        hidden = (jax.nn.silu(gate_act) * up_act).astype(jnp.bfloat16)
        result = jnp.dot(hidden, down_rows, preferred_element_type=jnp.float32).astype(jnp.bfloat16)
        result = result.reshape(block_count, CAP, D)
        contribution = weights_now[:, :, None] * result.astype(jnp.float32)
        accumulated = jax.vmap(add_rows)(accumulated, senders, contribution)
        return (accumulated, None)
    accumulated, unused = lax.scan(expert_step, blocks.astype(jnp.float32), jnp.arange(EXPERTS, dtype=jnp.int32))
    teacher = accumulated.astype(jnp.bfloat16)
    images_col = N_DP * IMG_DEV
    arranged = teacher.reshape(N_DP, N_EXPERT, IMG_DEV, IMG_TOK, D).transpose(1, 0, 2, 3, 4)
    arranged = arranged.reshape(N_EXPERT, images_col, IMG_TOK, D)
    targets = image_shard.reshape(N_DP, N_EXPERT, IMG_DEV).transpose(1, 0, 2).reshape(N_EXPERT, images_col)
    order_key = targets * images_col + jnp.arange(images_col, dtype=jnp.int32)[None, :]
    arrangement = jnp.argsort(order_key, axis=1).astype(jnp.int32)

    def pick_images(column_rows, column_order):
        return jnp.take(column_rows, column_order, axis=0)
    relaid = jax.vmap(pick_images)(arranged, arrangement)
    student_rows = relaid.reshape(N_EXPERT, N_DP, IMG_DEV, IMG_TOK, D).transpose(1, 0, 2, 3, 4).reshape(TOKENS, D)
    normed = normalize(student_rows, norm_gain)
    keys = jnp.dot(normed, key_proj, preferred_element_type=jnp.float32).astype(jnp.bfloat16)
    return (student_rows, keys)
```

```python
import functools

import jax
import jax.numpy as jnp
from jax import lax
from jax.experimental import pallas as pl
from jax.experimental.pallas import tpu as pltpu
from jax.sharding import PartitionSpec as P

IMG_TOK = 128


def normalize(values, norm_gain):
    wide = values.astype(jnp.float32)
    mean_square = jnp.mean(wide * wide, axis=-1, keepdims=True)
    return (wide * lax.rsqrt(mean_square + 1e-05) * norm_gain).astype(jnp.bfloat16)


def activate(incoming, gate_rows, up_rows):
    dims = (((1,), (1,)), ((), ()))
    gate_act = lax.dot_general(incoming, gate_rows, dims, preferred_element_type=jnp.float32)
    up_act = lax.dot_general(incoming, up_rows, dims, preferred_element_type=jnp.float32)
    return (jax.nn.silu(gate_act) * up_act).astype(jnp.bfloat16)


CHUNKS = 4
MESH = pl.DeviceIdType.MESH


def fused_kernel(
    n_expert,
    capacity,
    spread_ref,
    mix_ref,
    pick_ref,
    gain_ref,
    tokens_ref,
    gate_ref,
    up_ref,
    down_ref,
    key_ref,
    student_ref,
    keys_ref,
    gate_buf,
    up_buf,
    down_buf,
    key_buf,
    outgoing,
    incoming,
    produced,
    returned,
    tiles,
    hidden,
    normed,
    acc_gate,
    acc_up,
    send_sem,
    recv_sem,
    local_sem,
):
    d = lax.axis_index("dp")
    e = lax.axis_index("expert")
    dx = d + 1 - 2 * (d % 2)
    dy = (d + 2) % 4
    dd = (dx + 2) % 4
    core = e % 2
    sibling = e + 1 - 2 * core
    tok_dev, width = tokens_ref.shape
    units = gate_ref.shape[1]
    half_units = units // 2
    chunk = width // CHUNKS
    key_rows, key_width = key_ref.shape
    key_half = key_rows // 2
    key_quarter = key_rows // 4
    counts = {"remote": 0, "local": 0}

    def send(source, target, where):
        index = counts["remote"]
        counts["remote"] += 1
        copy = pltpu.make_async_remote_copy(
            src_ref=source,
            dst_ref=target,
            send_sem=send_sem.at[index],
            recv_sem=recv_sem.at[index],
            device_id=where,
            device_id_type=MESH,
        )
        copy.start()
        return copy

    def local(source, target):
        index = counts["local"]
        counts["local"] += 1
        copy = pltpu.make_async_copy(source, target, local_sem.at[index])
        copy.start()
        return copy

    to_x, to_y, to_sibling = {"dp": dx}, {"dp": dy}, {"expert": sibling}
    peers = [lax.rem(e + k, n_expert) for k in range(1, n_expert)]
    barrier = pltpu.get_barrier_semaphore()
    for where in [to_x, to_y] + [{"expert": peer} for peer in peers]:
        pl.semaphore_signal(barrier, inc=1, device_id=where, device_id_type=MESH)
    pl.semaphore_wait(barrier, n_expert + 1)
    sent = []

    def tracked(*args):
        copy = send(*args)
        sent.append(copy)
        return copy

    gate_x = tracked(gate_ref.at[0], gate_buf.at[1], to_x)
    gate_y = tracked(gate_ref.at[0], gate_buf.at[2], to_y)
    up_x = tracked(up_ref.at[0], up_buf.at[1], to_x)
    up_y = tracked(up_ref.at[0], up_buf.at[2], to_y)
    own_gate = local(gate_ref.at[0], gate_buf.at[0])
    own_up = local(up_ref.at[0], up_buf.at[0])
    own_down = local(down_ref.at[0], down_buf.at[0])
    own_key = local(key_ref, key_buf.at[0])

    step = 512
    spread = spread_ref[...]

    def fill(i, carry):
        cols = pl.ds(pl.multiple_of(i * step, step), step)
        rows = jnp.dot(spread, tokens_ref[:, cols], preferred_element_type=jnp.float32)
        outgoing[:, cols] = rows.astype(jnp.bfloat16)
        return carry

    lax.fori_loop(0, width // step, fill, 0)

    def rows_of(owner):
        return pl.ds(pl.multiple_of(owner * capacity, capacity), capacity)

    mine = rows_of(e)
    dispatched = [
        tracked(outgoing.at[rows_of(peer), :], incoming.at[mine, :], {"expert": peer})
        for peer in peers
    ]
    kept = local(outgoing.at[mine, :], incoming.at[mine, :])

    low, high = pl.ds(0, half_units), pl.ds(half_units, half_units)
    gate_y.wait_recv()
    gate_d0 = tracked(gate_buf.at[2, low, :], gate_buf.at[3, low, :], to_x)
    gate_x.wait_recv()
    gate_d1 = tracked(gate_buf.at[1, high, :], gate_buf.at[3, high, :], to_y)
    up_y.wait_recv()
    up_d0 = tracked(up_buf.at[2, low, :], up_buf.at[3, low, :], to_x)
    up_x.wait_recv()
    up_d1 = tracked(up_buf.at[1, high, :], up_buf.at[3, high, :], to_y)

    def down_own(c):
        cols = pl.ds(c * chunk, chunk)
        return (
            tracked(down_ref.at[0, :, cols], down_buf.at[1, :, cols], to_x),
            tracked(down_ref.at[0, :, cols], down_buf.at[2, :, cols], to_y),
        )

    downs = [down_own(0), down_own(1)]

    for copy in dispatched:
        copy.wait_recv()
    kept.wait()
    own_gate.wait()
    own_up.wait()
    dims = (((1,), (1,)), ((), ()))

    def activate_slot(slot):
        acc_gate[...] = jnp.zeros_like(acc_gate)
        acc_up[...] = jnp.zeros_like(acc_up)

        def add(i, carry):
            cols = pl.ds(pl.multiple_of(i * step, step), step)
            rows = incoming[:, cols]
            acc_gate[...] += lax.dot_general(
                rows, gate_buf[slot, :, cols], dims, preferred_element_type=jnp.float32
            )
            acc_up[...] += lax.dot_general(
                rows, up_buf[slot, :, cols], dims, preferred_element_type=jnp.float32
            )
            return carry

        lax.fori_loop(0, width // step, add, 0)
        gate_act = acc_gate[...]
        hidden[slot] = (gate_act / (1.0 + jnp.exp(-gate_act)) * acc_up[...]).astype(jnp.bfloat16)

    def activate_loop(slot, carry):
        activate_slot(slot)
        return carry

    lax.fori_loop(0, 3, activate_loop, 0)
    for copy in (gate_d0, gate_d1, up_d0, up_d1):
        copy.wait_recv()
    activate_slot(3)
    own_down.wait()

    narrow = 256
    hands = []
    key_copies = []
    my_half = pl.ds(pl.multiple_of(core * key_half, key_half), key_half)
    quarter0 = pl.ds(pl.multiple_of(core * key_half, key_quarter), key_quarter)
    quarter1 = pl.ds(pl.multiple_of(core * key_half + key_quarter, key_quarter), key_quarter)
    for c in range(CHUNKS):
        cols = pl.ds(c * chunk, chunk)
        down_x, down_y = downs[c]
        down_y.wait_recv()
        d0 = tracked(down_buf.at[2, low, cols], down_buf.at[3, low, cols], to_x)
        down_x.wait_recv()
        d1 = tracked(down_buf.at[1, high, cols], down_buf.at[3, high, cols], to_y)
        if c + 2 < CHUNKS:
            downs.append(down_own(c + 2))
        elif c + 1 == CHUNKS:
            key_copies.append(tracked(key_ref.at[my_half, :], key_buf.at[1, my_half, :], to_x))
            key_copies.append(tracked(key_ref.at[my_half, :], key_buf.at[2, my_half, :], to_y))
        d0.wait_recv()
        d1.wait_recv()

        def project(i, carry):
            at = pl.ds(pl.multiple_of(c * chunk + i * narrow, narrow), narrow)
            total = jnp.dot(hidden[0], down_buf[0, :, at], preferred_element_type=jnp.float32)
            for slot in range(1, 4):
                total += jnp.dot(
                    hidden[slot], down_buf[slot, :, at], preferred_element_type=jnp.float32
                )
            produced[:, at] = total.astype(jnp.bfloat16)
            return carry

        lax.fori_loop(0, chunk // narrow, project, 0)
        back = [
            tracked(produced.at[rows_of(peer), cols], returned.at[mine, cols], {"expert": peer})
            for peer in peers
        ]
        hands.append((back, local(produced.at[mine, cols], returned.at[mine, cols])))

    mix = mix_ref[...]
    mix_hi = mix.astype(jnp.bfloat16)
    mix_lo = (mix - mix_hi.astype(jnp.float32)).astype(jnp.bfloat16)
    half_tok = tok_dev // 2
    top, bottom = pl.ds(0, half_tok), pl.ds(half_tok, half_tok)
    tile_sends = []
    tile_diag = []

    def combine(c):
        back, own = hands[c]
        for copy in back:
            copy.wait_recv()
        own.wait()

        def blend(i, carry):
            at = pl.ds(pl.multiple_of(c * chunk + i * narrow, narrow), narrow)
            rows = returned[:, at]
            branch = jnp.dot(mix_hi, rows, preferred_element_type=jnp.float32)
            branch += jnp.dot(mix_lo, rows, preferred_element_type=jnp.float32)
            tiles[0, :, at] = (tokens_ref[:, at].astype(jnp.float32) + branch).astype(jnp.bfloat16)
            return carry

        lax.fori_loop(0, chunk // narrow, blend, 0)
        cols = pl.ds(c * chunk, chunk)
        tile_sends.append(
            (
                tracked(tiles.at[0, :, cols], tiles.at[1, :, cols], to_x),
                tracked(tiles.at[0, :, cols], tiles.at[2, :, cols], to_y),
            )
        )

    def relay(c):
        cols = pl.ds(c * chunk, chunk)
        tile_x, tile_y = tile_sends[c]
        tile_y.wait_recv()
        tile_diag.append(tracked(tiles.at[2, top, cols], tiles.at[3, top, cols], to_x))
        tile_x.wait_recv()
        tile_diag.append(tracked(tiles.at[1, bottom, cols], tiles.at[3, bottom, cols], to_y))

    shared = []

    def share(slot, rows):
        shared.append(tracked(key_buf.at[slot, rows, :], key_buf.at[slot, rows, :], to_sibling))

    combine(0)
    key_x, key_y = key_copies
    key_y.wait_recv()
    key_d0 = tracked(key_buf.at[2, quarter0, :], key_buf.at[3, quarter0, :], to_x)
    share(2, my_half)
    key_x.wait_recv()
    key_d1 = tracked(key_buf.at[1, quarter1, :], key_buf.at[3, quarter1, :], to_y)
    share(1, my_half)
    combine(1)
    relay(0)
    combine(2)
    relay(1)
    key_d0.wait_recv()
    share(3, quarter0)
    key_d1.wait_recv()
    share(3, quarter1)
    combine(3)
    relay(2)
    relay(3)
    for copy in tile_diag:
        copy.wait_recv()

    def choose(i, squares):
        at = pl.ds(pl.multiple_of(i * narrow, narrow), narrow)
        rows = pick_ref[0, :, 0:1] * tiles[0, :, at].astype(jnp.float32)
        for slot in range(1, 4):
            rows += pick_ref[slot, :, 0:1] * tiles[slot, :, at].astype(jnp.float32)
        student_ref[:, at] = rows.astype(jnp.bfloat16)
        return squares + jnp.sum(rows * rows, axis=-1, keepdims=True)

    squares = lax.fori_loop(0, width // narrow, choose, jnp.zeros((tok_dev, 1), jnp.float32))
    scale = lax.rsqrt(squares / width + 1e-05)

    def norm(i, carry):
        at = pl.ds(pl.multiple_of(i * narrow, narrow), narrow)
        rows = student_ref[:, at].astype(jnp.float32)
        normed[:, at] = (rows * scale * gain_ref[:, at]).astype(jnp.bfloat16)
        return carry

    lax.fori_loop(0, width // narrow, norm, 0)
    own_key.wait()
    for copy in shared:
        copy.wait_recv()
    columns = [
        normed[:, pl.ds(pl.multiple_of(owner * key_rows, key_rows), key_rows)]
        for owner in (d, dx, dy, dd)
    ]

    def to_keys(i, carry):
        at = pl.ds(pl.multiple_of(i * narrow, narrow), narrow)
        total = jnp.dot(columns[0], key_buf[0, :, at], preferred_element_type=jnp.float32)
        for slot in range(1, 4):
            total += jnp.dot(columns[slot], key_buf[slot, :, at], preferred_element_type=jnp.float32)
        keys_ref[:, at] = total.astype(jnp.bfloat16)
        return carry

    lax.fori_loop(0, key_width // narrow, to_keys, 0)
    for copy in sent:
        copy.wait_send()


def fused(
    tokens,
    gate_proj,
    up_proj,
    down_proj,
    route_ids,
    route_slots,
    route_gates,
    image_shard,
    norm_gain,
    key_proj,
    capacity,
):
    tok_dev, width = tokens.shape
    n_expert = lax.axis_size("expert")
    slots = n_expert * capacity
    units = gate_proj.shape[1]
    key_rows, key_width = key_proj.shape
    retained = route_slots < capacity
    cells = jnp.where(retained, route_ids * capacity + route_slots, slots)
    grid = jnp.arange(slots, dtype=jnp.int32)
    spread = jnp.any(cells.T[:, None, :] == grid[None, :, None], axis=0).astype(jnp.bfloat16)
    mix = jnp.sum(
        jnp.where(cells[:, :, None] == grid[None, None, :], route_gates[:, :, None], 0.0), axis=1
    )
    d = lax.axis_index("dp")
    dx = d + 1 - 2 * (d % 2)
    order = jnp.stack([d, dx, (d + 2) % 4, (dx + 2) % 4])
    pick = (jnp.take(image_shard.reshape(-1), order) == d).astype(jnp.float32)
    pick = jnp.broadcast_to(pick[:, None, None], (4, tok_dev, 128))
    remote = 8 + (n_expert - 1) * (1 + CHUNKS) + 4 * CHUNKS * 2 + 8
    vmem = pl.BlockSpec(memory_space=pltpu.VMEM)
    anywhere = pl.BlockSpec(memory_space=pl.ANY)
    half = jnp.bfloat16
    return pl.pallas_call(
        functools.partial(fused_kernel, n_expert, capacity),
        out_shape=(
            jax.ShapeDtypeStruct((tok_dev, width), half),
            jax.ShapeDtypeStruct((tok_dev, key_width), half),
        ),
        in_specs=[vmem] * 5 + [anywhere] * 4,
        out_specs=(vmem, vmem),
        scratch_shapes=[
            pltpu.VMEM((4, units, width), half),
            pltpu.VMEM((4, units, width), half),
            pltpu.VMEM((4, units, width), half),
            pltpu.VMEM((4, key_rows, key_width), half),
            pltpu.VMEM((slots, width), half),
            pltpu.VMEM((slots, width), half),
            pltpu.VMEM((slots, width), half),
            pltpu.VMEM((slots, width), half),
            pltpu.VMEM((4, tok_dev, width), half),
            pltpu.VMEM((4, slots, units), half),
            pltpu.VMEM((tok_dev, width), half),
            pltpu.VMEM((slots, units), jnp.float32),
            pltpu.VMEM((slots, units), jnp.float32),
            pltpu.SemaphoreType.DMA((remote,)),
            pltpu.SemaphoreType.DMA((remote,)),
            pltpu.SemaphoreType.DMA((5 + CHUNKS,)),
        ],
        compiler_params=pltpu.CompilerParams(
            collective_id=0, has_side_effects=True, vmem_limit_bytes=60 * 1024 * 1024
        ),
    )(
        spread,
        mix,
        pick,
        norm_gain.reshape(1, -1),
        tokens,
        gate_proj,
        up_proj,
        down_proj,
        key_proj,
    )


def per_device(
    tokens,
    gate_proj,
    up_proj,
    down_proj,
    route_ids,
    route_slots,
    route_gates,
    image_shard,
    norm_gain,
    key_proj,
):
    tok_dev, model_width = tokens.shape
    top_count = route_ids.shape[1]
    experts = gate_proj.shape[0] * lax.axis_size("expert")
    capacity = 3 * tok_dev * top_count // (2 * experts)
    if capacity % 16 == 0 and gate_proj.shape[0] == 1 and lax.axis_size("dp") == 4:
        if tok_dev == IMG_TOK and gate_proj.shape[1] % 32 == 0 and key_proj.shape[0] % 128 == 0:
            return fused(
                tokens,
                gate_proj,
                up_proj,
                down_proj,
                route_ids,
                route_slots,
                route_gates,
                image_shard,
                norm_gain,
                key_proj,
                capacity,
            )
    slot_total = experts * capacity
    retained = route_slots < capacity
    slot_cells = jnp.where(retained, route_ids * capacity + route_slots, slot_total).reshape(-1)
    owners = jnp.arange(tok_dev * top_count, dtype=jnp.int32) // top_count
    cell_token = (
        jnp.full((slot_total + 1,), tok_dev, jnp.int32).at[slot_cells].set(owners)[:slot_total]
    )
    outgoing = jnp.take(tokens, cell_token, axis=0, mode="fill", fill_value=0).reshape(
        experts, capacity, model_width
    )
    arrived = lax.all_to_all(outgoing, "expert", split_axis=0, concat_axis=0, tiled=True)
    incoming = arrived.reshape(-1, model_width)
    hidden = activate(
        incoming,
        lax.all_gather(gate_proj, "dp", axis=1, tiled=True)[0],
        lax.all_gather(up_proj, "dp", axis=1, tiled=True)[0],
    )
    summed = jnp.dot(
        hidden,
        lax.all_gather(down_proj, "dp", axis=1, tiled=True)[0],
        preferred_element_type=jnp.float32,
    )
    produced = summed.astype(jnp.bfloat16).reshape(arrived.shape)
    returned = lax.all_to_all(produced, "expert", split_axis=0, concat_axis=0, tiled=True).reshape(
        -1, model_width
    )
    picked = jnp.take(returned, slot_cells, axis=0, mode="fill", fill_value=0).reshape(
        tok_dev, top_count, model_width
    )
    mixing = jnp.where(retained, route_gates, 0.0)
    branch = jnp.einsum("tk,tkd->td", mixing, picked.astype(jnp.float32))
    teacher = (tokens.astype(jnp.float32) + branch).astype(jnp.bfloat16)
    gathered = lax.all_gather(teacher, "dp", axis=0, tiled=True)
    shard_column = image_shard.reshape(-1)
    images_col = shard_column.shape[0]
    arrangement = jnp.argsort(shard_column * images_col + jnp.arange(images_col, dtype=jnp.int32))
    images = gathered.reshape(images_col, IMG_TOK, model_width)
    position = lax.axis_index("dp")
    ordered = jnp.take(images, arrangement, axis=0).reshape(images_col * IMG_TOK, model_width)
    student_rows = lax.dynamic_slice_in_dim(ordered, position * tok_dev, tok_dev, 0)
    normed = normalize(ordered, norm_gain)
    columns = lax.dynamic_slice_in_dim(normed, position * key_proj.shape[0], key_proj.shape[0], 1)
    projected = lax.psum_scatter(
        jnp.dot(columns, key_proj, preferred_element_type=jnp.float32),
        "dp",
        scatter_dimension=0,
        tiled=True,
    )
    return (student_rows, projected.astype(jnp.bfloat16))


def solution(mesh):
    in_specs = (
        P(("dp", "expert"), None),
        P("expert", "dp", None),
        P("expert", "dp", None),
        P("expert", "dp", None),
        P(("dp", "expert"), None),
        P(("dp", "expert"), None),
        P(("dp", "expert"), None),
        P(None, "expert"),
        P(),
        P("dp", None),
    )
    out_specs = (P(("dp", "expert"), None), P(("dp", "expert"), None))
    return jax.shard_map(
        per_device, mesh=mesh, in_specs=in_specs, out_specs=out_specs, check_vma=False
    )
```

```python
import functools

import jax
import jax.numpy as jnp
from jax import lax
from jax.experimental import pallas as pl
from jax.experimental.pallas import tpu as pltpu
from jax.sharding import PartitionSpec as P

IMG_TOK = 128


def normalize(values, norm_gain):
    wide = values.astype(jnp.float32)
    mean_square = jnp.mean(wide * wide, axis=-1, keepdims=True)
    return (wide * lax.rsqrt(mean_square + 1e-05) * norm_gain).astype(jnp.bfloat16)


def activate(incoming, gate_rows, up_rows):
    dims = (((1,), (1,)), ((), ()))
    gate_act = lax.dot_general(incoming, gate_rows, dims, preferred_element_type=jnp.float32)
    up_act = lax.dot_general(incoming, up_rows, dims, preferred_element_type=jnp.float32)
    return (jax.nn.silu(gate_act) * up_act).astype(jnp.bfloat16)


CHUNKS = 8
PIECES = 2
LAG = 3
MESH = pl.DeviceIdType.MESH


def fused_kernel(
    n_expert,
    capacity,
    ids_ref,
    slots_ref,
    gates_ref,
    shard_ref,
    gain_ref,
    tokens_ref,
    gate_ref,
    up_ref,
    down_ref,
    key_ref,
    student_ref,
    keys_ref,
    gate_buf,
    up_buf,
    down_buf,
    key_buf,
    outgoing,
    incoming,
    produced,
    returned,
    tiles,
    passed,
    hidden,
    gained,
    mixing,
    acc_keys,
    acc_gate,
    acc_up,
    squares,
    send_sem,
    recv_sem,
    local_sem,
):
    d = lax.axis_index("dp")
    e = lax.axis_index("expert")
    dx = d + 1 - 2 * (d % 2)
    dy = (d + 2) % 4
    dd = (dx + 2) % 4
    core = e % 2
    sibling = e + 1 - 2 * core
    partner = e + 2 - 4 * ((e // 2) % 2)
    tok_dev, width = tokens_ref.shape
    units = gate_ref.shape[1]
    half_units = units // 2
    chunk = width // CHUNKS
    key_rows, key_width = key_ref.shape
    quarter = key_rows // 4
    piece = quarter // PIECES
    half_piece = piece // 2
    slots = n_expert * capacity
    counts = {"remote": 0, "local": 0}

    def send(source, target, where):
        index = counts["remote"]
        counts["remote"] += 1
        copy = pltpu.make_async_remote_copy(
            src_ref=source,
            dst_ref=target,
            send_sem=send_sem.at[index],
            recv_sem=recv_sem.at[index],
            device_id=where,
            device_id_type=MESH,
        )
        copy.start()
        return copy

    def local(source, target):
        index = counts["local"]
        counts["local"] += 1
        copy = pltpu.make_async_copy(source, target, local_sem.at[index])
        copy.start()
        return copy

    to_x, to_y, to_sibling = {"dp": dx}, {"dp": dy}, {"expert": sibling}
    to_partner = {"expert": partner}
    peers = [lax.rem(e + k, n_expert) for k in range(1, n_expert)]
    barrier = pltpu.get_barrier_semaphore()
    for where in [to_x, to_y] + [{"expert": peer} for peer in peers]:
        pl.semaphore_signal(barrier, inc=1, device_id=where, device_id_type=MESH)
    pl.semaphore_wait(barrier, n_expert + 1)
    sent = []

    def tracked(*args):
        copy = send(*args)
        sent.append(copy)
        return copy

    gate_x = tracked(gate_ref.at[0], gate_buf.at[1], to_x)
    gate_y = tracked(gate_ref.at[0], gate_buf.at[2], to_y)
    up_x = tracked(up_ref.at[0], up_buf.at[1], to_x)
    up_y = tracked(up_ref.at[0], up_buf.at[2], to_y)
    own_gate = local(gate_ref.at[0], gate_buf.at[0])
    own_up = local(up_ref.at[0], up_buf.at[0])
    own_down = local(down_ref.at[0], down_buf.at[0])
    own_key = local(key_ref, key_buf.at[d])

    step = 512
    grid = lax.broadcasted_iota(jnp.int32, (tok_dev, slots), 1)
    mix = jnp.zeros((tok_dev, slots), jnp.float32)
    named = jnp.zeros((tok_dev, slots), jnp.float32)
    for k in range(ids_ref.shape[1]):
        queue = slots_ref[:, k : k + 1]
        cell = jnp.where(queue < capacity, ids_ref[:, k : k + 1] * capacity + queue, slots)
        hit = grid == cell
        mix += jnp.where(hit, gates_ref[:, k : k + 1], 0.0)
        named += jnp.where(hit, 1.0, 0.0)
    mixing[...] = mix
    spread = named.T.astype(jnp.bfloat16)

    def fill(i, carry):
        cols = pl.ds(pl.multiple_of(i * step, step), step)
        rows = jnp.dot(spread, tokens_ref[:, cols], preferred_element_type=jnp.float32)
        outgoing[:, cols] = rows.astype(jnp.bfloat16)
        return carry

    lax.fori_loop(0, width // step, fill, 0)

    def rows_of(owner):
        return pl.ds(pl.multiple_of(owner * capacity, capacity), capacity)

    mine = rows_of(e)
    dispatched = [
        tracked(outgoing.at[rows_of(peer), :], incoming.at[mine, :], {"expert": peer})
        for peer in peers
    ]
    kept = local(outgoing.at[mine, :], incoming.at[mine, :])

    low, high = pl.ds(0, half_units), pl.ds(half_units, half_units)
    gate_y.wait_recv()
    gate_d0 = tracked(gate_buf.at[2, low, :], gate_buf.at[3, low, :], to_x)
    gate_x.wait_recv()
    gate_d1 = tracked(gate_buf.at[1, high, :], gate_buf.at[3, high, :], to_y)
    up_y.wait_recv()
    up_d0 = tracked(up_buf.at[2, low, :], up_buf.at[3, low, :], to_x)
    up_x.wait_recv()
    up_d1 = tracked(up_buf.at[1, high, :], up_buf.at[3, high, :], to_y)

    def down_own(c):
        cols = pl.ds(c * chunk, chunk)
        return (
            tracked(down_ref.at[0, :, cols], down_buf.at[1, :, cols], to_x),
            tracked(down_ref.at[0, :, cols], down_buf.at[2, :, cols], to_y),
        )

    def key_rows_at(owner, p, start=0, size=piece):
        first = (owner % 4) * quarter + p * piece + start
        return pl.ds(pl.multiple_of(first, half_piece), size)

    def key_own(p):
        rows = key_rows_at(e, p)
        return (
            tracked(key_ref.at[rows, :], key_buf.at[d, rows, :], to_x),
            tracked(key_ref.at[rows, :], key_buf.at[d, rows, :], to_y),
        )

    key_first, key_second, key_across, key_shared = [], [], [], []

    def pass_key(owner, rows, where):
        part = key_buf.at[owner, rows, :]
        return tracked(part, part, where)

    def key_share(owner, rows):
        key_across.append(pass_key(owner, rows, to_partner))
        key_shared.append(pass_key(owner, rows, to_sibling))

    def key_middle(p):
        key_x, key_y = key_first[p]
        rows = key_rows_at(e, p)
        key_y.wait_recv()
        d0 = pass_key(dy, key_rows_at(e, p, 0, half_piece), to_x)
        key_x.wait_recv()
        d1 = pass_key(dx, key_rows_at(e, p, half_piece, half_piece), to_y)
        key_second.append((d0, d1))
        key_share(dy, rows)
        key_share(dx, rows)

    def key_diagonal(p):
        d0, d1 = key_second[p]
        d0.wait_recv()
        key_share(dd, key_rows_at(e, p, 0, half_piece))
        d1.wait_recv()
        key_share(dd, key_rows_at(e, p, half_piece, half_piece))

    def key_onward(p, halves):
        copies = key_across[4 * p + 2 * halves : 4 * p + 2 * halves + 2]
        if halves:
            places = [
                (dd, key_rows_at(partner, p, 0, half_piece)),
                (dd, key_rows_at(partner, p, half_piece, half_piece)),
            ]
        else:
            places = [(dy, key_rows_at(partner, p)), (dx, key_rows_at(partner, p))]
        for copy, (owner, rows) in zip(copies, places):
            copy.wait_recv()
            key_shared.append(pass_key(owner, rows, to_sibling))

    downs = [down_own(0), down_own(1)]
    key_first.append(key_own(0))

    for copy in dispatched:
        copy.wait_recv()
    kept.wait()
    own_gate.wait()
    own_up.wait()
    dims = (((1,), (1,)), ((), ()))

    def activate_slot(slot):
        acc_gate[...] = jnp.zeros_like(acc_gate)
        acc_up[...] = jnp.zeros_like(acc_up)

        def add(i, carry):
            cols = pl.ds(pl.multiple_of(i * step, step), step)
            rows = incoming[:, cols]
            acc_gate[...] += lax.dot_general(
                rows, gate_buf[slot, :, cols], dims, preferred_element_type=jnp.float32
            )
            acc_up[...] += lax.dot_general(
                rows, up_buf[slot, :, cols], dims, preferred_element_type=jnp.float32
            )
            return carry

        lax.fori_loop(0, width // step, add, 0)
        gate_act = acc_gate[...]
        hidden[slot] = (gate_act / (1.0 + jnp.exp(-gate_act)) * acc_up[...]).astype(jnp.bfloat16)

    def activate_loop(slot, carry):
        activate_slot(slot)
        return carry

    lax.fori_loop(0, 3, activate_loop, 0)
    for copy in (gate_d0, gate_d1, up_d0, up_d1):
        copy.wait_recv()
    activate_slot(3)
    own_down.wait()

    narrow = 256
    hands = []
    tile_first, tile_second = [], []
    acc_keys[...] = jnp.zeros_like(acc_keys)
    squares[...] = jnp.zeros_like(squares)

    def flag(owner, shard):
        return jnp.where(shard_ref[owner, 0] == shard, 1.0, 0.0)

    def ways(c):
        return (dx, dy, to_x, to_y) if c % 2 == 0 else (dy, dx, to_y, to_x)

    def combine(c):
        back, own = hands[c]
        for copy in back:
            copy.wait_recv()
        own.wait()
        mix = mixing[...]
        mix_hi = mix.astype(jnp.bfloat16)
        mix_lo = (mix - mix_hi.astype(jnp.float32)).astype(jnp.bfloat16)

        def blend(i, carry):
            at = pl.ds(pl.multiple_of(c * chunk + i * narrow, narrow), narrow)
            rows = returned[:, at]
            branch = jnp.dot(mix_hi, rows, preferred_element_type=jnp.float32)
            branch += jnp.dot(mix_lo, rows, preferred_element_type=jnp.float32)
            tiles[0, :, at] = (tokens_ref[:, at].astype(jnp.float32) + branch).astype(jnp.bfloat16)
            return carry

        lax.fori_loop(0, chunk // narrow, blend, 0)
        cols = pl.ds(c * chunk, chunk)
        tile_first.append(tracked(tiles.at[0, :, cols], tiles.at[1, :, cols], ways(c)[2]))

    def swap(c):
        near, far, _, to_far = ways(c)
        own = flag(d, far)
        tile_first[c].wait_recv()

        def mask(i, carry):
            at = pl.ds(pl.multiple_of(c * chunk + i * narrow, narrow), narrow)
            rows = own * tiles[0, :, at].astype(jnp.float32)
            rows += (1.0 - own) * tiles[1, :, at].astype(jnp.float32)
            passed[:, at] = rows.astype(jnp.bfloat16)
            return carry

        lax.fori_loop(0, chunk // narrow, mask, 0)
        cols = pl.ds(c * chunk, chunk)
        tile_second.append(tracked(passed.at[:, cols], tiles.at[2, :, cols], to_far))

    def finish(c):
        near = ways(c)[0]
        weights = [flag(d, d), flag(near, d)]
        weights.append(1.0 - weights[0] - weights[1])
        tile_second[c].wait_recv()

        def choose(i, carry):
            at = pl.ds(pl.multiple_of(c * chunk + i * narrow, narrow), narrow)
            rows = weights[0] * tiles[0, :, at].astype(jnp.float32)
            for slot in (1, 2):
                rows += weights[slot] * tiles[slot, :, at].astype(jnp.float32)
            student_ref[:, at] = rows.astype(jnp.bfloat16)
            gained[:, at] = (rows * gain_ref[:, at]).astype(jnp.bfloat16)
            squares[...] += jnp.sum(rows * rows, axis=-1, keepdims=True)
            return carry

        lax.fori_loop(0, chunk // narrow, choose, 0)

    def project_keys(c, carry):
        at = pl.ds(pl.multiple_of(c * chunk, chunk), chunk)
        per_owner = key_rows // chunk
        rows = pl.ds(pl.multiple_of((c % per_owner) * chunk, chunk), chunk)
        acc_keys[...] += jnp.dot(
            gained[:, at], key_buf[c // per_owner, rows, :], preferred_element_type=jnp.float32
        )
        return carry

    def follow(c):
        if 0 <= c - LAG < CHUNKS:
            combine(c - LAG)
        if 0 <= c - LAG - 1 < CHUNKS:
            swap(c - LAG - 1)
        if 0 <= c - LAG - 2 < CHUNKS:
            finish(c - LAG - 2)

    for c in range(CHUNKS):
        cols = pl.ds(c * chunk, chunk)
        down_x, down_y = downs[c]
        down_y.wait_recv()
        d0 = tracked(down_buf.at[2, low, cols], down_buf.at[3, low, cols], to_x)
        down_x.wait_recv()
        d1 = tracked(down_buf.at[1, high, cols], down_buf.at[3, high, cols], to_y)
        if c + 2 < CHUNKS:
            downs.append(down_own(c + 2))
        if c == 1:
            key_first.append(key_own(1))
        d0.wait_recv()
        d1.wait_recv()

        def project(i, carry):
            at = pl.ds(pl.multiple_of(c * chunk + i * narrow, narrow), narrow)
            total = jnp.dot(hidden[0], down_buf[0, :, at], preferred_element_type=jnp.float32)
            for slot in range(1, 4):
                total += jnp.dot(
                    hidden[slot], down_buf[slot, :, at], preferred_element_type=jnp.float32
                )
            produced[:, at] = total.astype(jnp.bfloat16)
            return carry

        lax.fori_loop(0, chunk // narrow, project, 0)
        back = [
            tracked(produced.at[rows_of(peer), cols], returned.at[mine, cols], {"expert": peer})
            for peer in peers
        ]
        hands.append((back, local(produced.at[mine, cols], returned.at[mine, cols])))

        if c == 2:
            key_middle(0)
        if c == 4:
            key_diagonal(0)
            key_middle(1)
        if c == 6:
            key_diagonal(1)
            key_onward(0, 0)
        follow(c)

    key_onward(0, 1)
    key_onward(1, 0)
    follow(CHUNKS)
    key_onward(1, 1)
    follow(CHUNKS + 1)
    own_key.wait()
    for copy in key_shared:
        copy.wait_recv()
    ready = CHUNKS + 2 - LAG - 2
    lax.fori_loop(0, ready, project_keys, 0)
    for c in range(CHUNKS + 2, CHUNKS + LAG + 2):
        follow(c)
        project_keys(c - LAG - 2, 0)
    scale = lax.rsqrt(squares[...] / width + 1e-05)
    keys_ref[...] = (acc_keys[...] * scale).astype(jnp.bfloat16)
    for copy in sent:
        copy.wait_send()


def fused(
    tokens,
    gate_proj,
    up_proj,
    down_proj,
    route_ids,
    route_slots,
    route_gates,
    image_shard,
    norm_gain,
    key_proj,
    capacity,
):
    tok_dev, width = tokens.shape
    n_expert = lax.axis_size("expert")
    slots = n_expert * capacity
    units = gate_proj.shape[1]
    key_rows, key_width = key_proj.shape
    remote = 8 + 16 * PIECES + (n_expert - 1) * (1 + CHUNKS) + 6 * CHUNKS
    vmem = pl.BlockSpec(memory_space=pltpu.VMEM)
    anywhere = pl.BlockSpec(memory_space=pl.ANY)
    scalars = pl.BlockSpec(memory_space=pltpu.SMEM)
    half = jnp.bfloat16
    return pl.pallas_call(
        functools.partial(fused_kernel, n_expert, capacity),
        out_shape=(
            jax.ShapeDtypeStruct((tok_dev, width), half),
            jax.ShapeDtypeStruct((tok_dev, key_width), half),
        ),
        in_specs=[vmem] * 3 + [scalars] + [vmem] * 2 + [anywhere] * 4,
        out_specs=(vmem, vmem),
        scratch_shapes=[
            pltpu.VMEM((4, units, width), half),
            pltpu.VMEM((4, units, width), half),
            pltpu.VMEM((4, units, width), half),
            pltpu.VMEM((4, key_rows, key_width), half),
            pltpu.VMEM((slots, width), half),
            pltpu.VMEM((slots, width), half),
            pltpu.VMEM((slots, width), half),
            pltpu.VMEM((slots, width), half),
            pltpu.VMEM((3, tok_dev, width), half),
            pltpu.VMEM((tok_dev, width), half),
            pltpu.VMEM((4, slots, units), half),
            pltpu.VMEM((tok_dev, width), half),
            pltpu.VMEM((tok_dev, slots), jnp.float32),
            pltpu.VMEM((tok_dev, key_width), jnp.float32),
            pltpu.VMEM((slots, units), jnp.float32),
            pltpu.VMEM((slots, units), jnp.float32),
            pltpu.VMEM((tok_dev, 1), jnp.float32),
            pltpu.SemaphoreType.DMA((remote,)),
            pltpu.SemaphoreType.DMA((remote,)),
            pltpu.SemaphoreType.DMA((5 + CHUNKS,)),
        ],
        compiler_params=pltpu.CompilerParams(
            collective_id=0, has_side_effects=True, vmem_limit_bytes=60 * 1024 * 1024
        ),
    )(
        route_ids,
        route_slots,
        route_gates,
        image_shard,
        norm_gain.reshape(1, -1),
        tokens,
        gate_proj,
        up_proj,
        down_proj,
        key_proj,
    )


def per_device(
    tokens,
    gate_proj,
    up_proj,
    down_proj,
    route_ids,
    route_slots,
    route_gates,
    image_shard,
    norm_gain,
    key_proj,
):
    tok_dev, model_width = tokens.shape
    top_count = route_ids.shape[1]
    experts = gate_proj.shape[0] * lax.axis_size("expert")
    capacity = 3 * tok_dev * top_count // (2 * experts)
    if capacity % 16 == 0 and gate_proj.shape[0] == 1 and lax.axis_size("dp") == 4 and experts % 4 == 0:
        if tok_dev == IMG_TOK and gate_proj.shape[1] % 32 == 0 and key_proj.shape[0] % 512 == 0:
            return fused(
                tokens,
                gate_proj,
                up_proj,
                down_proj,
                route_ids,
                route_slots,
                route_gates,
                image_shard,
                norm_gain,
                key_proj,
                capacity,
            )
    slot_total = experts * capacity
    retained = route_slots < capacity
    slot_cells = jnp.where(retained, route_ids * capacity + route_slots, slot_total).reshape(-1)
    owners = jnp.arange(tok_dev * top_count, dtype=jnp.int32) // top_count
    cell_token = (
        jnp.full((slot_total + 1,), tok_dev, jnp.int32).at[slot_cells].set(owners)[:slot_total]
    )
    outgoing = jnp.take(tokens, cell_token, axis=0, mode="fill", fill_value=0).reshape(
        experts, capacity, model_width
    )
    arrived = lax.all_to_all(outgoing, "expert", split_axis=0, concat_axis=0, tiled=True)
    incoming = arrived.reshape(-1, model_width)
    hidden = activate(
        incoming,
        lax.all_gather(gate_proj, "dp", axis=1, tiled=True)[0],
        lax.all_gather(up_proj, "dp", axis=1, tiled=True)[0],
    )
    summed = jnp.dot(
        hidden,
        lax.all_gather(down_proj, "dp", axis=1, tiled=True)[0],
        preferred_element_type=jnp.float32,
    )
    produced = summed.astype(jnp.bfloat16).reshape(arrived.shape)
    returned = lax.all_to_all(produced, "expert", split_axis=0, concat_axis=0, tiled=True).reshape(
        -1, model_width
    )
    picked = jnp.take(returned, slot_cells, axis=0, mode="fill", fill_value=0).reshape(
        tok_dev, top_count, model_width
    )
    mixing = jnp.where(retained, route_gates, 0.0)
    branch = jnp.einsum("tk,tkd->td", mixing, picked.astype(jnp.float32))
    teacher = (tokens.astype(jnp.float32) + branch).astype(jnp.bfloat16)
    gathered = lax.all_gather(teacher, "dp", axis=0, tiled=True)
    shard_column = image_shard.reshape(-1)
    images_col = shard_column.shape[0]
    arrangement = jnp.argsort(shard_column * images_col + jnp.arange(images_col, dtype=jnp.int32))
    images = gathered.reshape(images_col, IMG_TOK, model_width)
    position = lax.axis_index("dp")
    ordered = jnp.take(images, arrangement, axis=0).reshape(images_col * IMG_TOK, model_width)
    student_rows = lax.dynamic_slice_in_dim(ordered, position * tok_dev, tok_dev, 0)
    normed = normalize(ordered, norm_gain)
    columns = lax.dynamic_slice_in_dim(normed, position * key_proj.shape[0], key_proj.shape[0], 1)
    projected = lax.psum_scatter(
        jnp.dot(columns, key_proj, preferred_element_type=jnp.float32),
        "dp",
        scatter_dimension=0,
        tiled=True,
    )
    return (student_rows, projected.astype(jnp.bfloat16))


def solution(mesh):
    in_specs = (
        P(("dp", "expert"), None),
        P("expert", "dp", None),
        P("expert", "dp", None),
        P("expert", "dp", None),
        P(("dp", "expert"), None),
        P(("dp", "expert"), None),
        P(("dp", "expert"), None),
        P(None, "expert"),
        P(),
        P("dp", None),
    )
    out_specs = (P(("dp", "expert"), None), P(("dp", "expert"), None))
    return jax.shard_map(
        per_device, mesh=mesh, in_specs=in_specs, out_specs=out_specs, check_vma=False
    )
```

```python
import functools

import jax
import jax.numpy as jnp
from jax import lax
from jax.experimental import pallas as pl
from jax.experimental.pallas import tpu as pltpu
from jax.sharding import PartitionSpec as P

IMG_TOK = 128


def normalize(values, norm_gain):
    wide = values.astype(jnp.float32)
    mean_square = jnp.mean(wide * wide, axis=-1, keepdims=True)
    return (wide * lax.rsqrt(mean_square + 1e-05) * norm_gain).astype(jnp.bfloat16)


def activate(incoming, gate_rows, up_rows):
    dims = (((1,), (1,)), ((), ()))
    gate_act = lax.dot_general(incoming, gate_rows, dims, preferred_element_type=jnp.float32)
    up_act = lax.dot_general(incoming, up_rows, dims, preferred_element_type=jnp.float32)
    return (jax.nn.silu(gate_act) * up_act).astype(jnp.bfloat16)


CHUNKS = 4
PIECES = 2
LAG = 2
MESH = pl.DeviceIdType.MESH


def fused_kernel(
    n_expert,
    capacity,
    ids_ref,
    slots_ref,
    gates_ref,
    shard_ref,
    gain_ref,
    tokens_ref,
    gate_ref,
    up_ref,
    down_ref,
    key_ref,
    student_ref,
    keys_ref,
    gate_buf,
    up_buf,
    down_buf,
    key_buf,
    outgoing,
    incoming,
    produced,
    returned,
    tiles,
    passed,
    hidden,
    gained,
    mixing,
    acc_keys,
    acc_gate,
    acc_up,
    squares,
    send_sem,
    recv_sem,
    local_sem,
):
    d = lax.axis_index("dp")
    e = lax.axis_index("expert")
    dx = d + 1 - 2 * (d % 2)
    dy = (d + 2) % 4
    dd = (dx + 2) % 4
    core = e % 2
    sibling = e + 1 - 2 * core
    tok_dev, width = tokens_ref.shape
    units = gate_ref.shape[1]
    half_units = units // 2
    chunk = width // CHUNKS
    key_rows, key_width = key_ref.shape
    key_half = key_rows // 2
    piece = key_half // PIECES
    half_piece = piece // 2
    slots = n_expert * capacity
    counts = {"remote": 0, "local": 0}

    def send(source, target, where):
        index = counts["remote"]
        counts["remote"] += 1
        copy = pltpu.make_async_remote_copy(
            src_ref=source,
            dst_ref=target,
            send_sem=send_sem.at[index],
            recv_sem=recv_sem.at[index],
            device_id=where,
            device_id_type=MESH,
        )
        copy.start()
        return copy

    def local(source, target):
        index = counts["local"]
        counts["local"] += 1
        copy = pltpu.make_async_copy(source, target, local_sem.at[index])
        copy.start()
        return copy

    to_x, to_y, to_sibling = {"dp": dx}, {"dp": dy}, {"expert": sibling}
    peers = [lax.rem(e + k, n_expert) for k in range(1, n_expert)]
    barrier = pltpu.get_barrier_semaphore()
    for where in [to_x, to_y] + [{"expert": peer} for peer in peers]:
        pl.semaphore_signal(barrier, inc=1, device_id=where, device_id_type=MESH)
    pl.semaphore_wait(barrier, n_expert + 1)
    sent = []

    def tracked(*args):
        copy = send(*args)
        sent.append(copy)
        return copy

    gate_x = tracked(gate_ref.at[0], gate_buf.at[1], to_x)
    gate_y = tracked(gate_ref.at[0], gate_buf.at[2], to_y)
    up_x = tracked(up_ref.at[0], up_buf.at[1], to_x)
    up_y = tracked(up_ref.at[0], up_buf.at[2], to_y)
    own_gate = local(gate_ref.at[0], gate_buf.at[0])
    own_up = local(up_ref.at[0], up_buf.at[0])
    own_down = local(down_ref.at[0], down_buf.at[0])
    own_key = local(key_ref, key_buf.at[d])

    step = 512
    grid = lax.broadcasted_iota(jnp.int32, (tok_dev, slots), 1)
    mix = jnp.zeros((tok_dev, slots), jnp.float32)
    named = jnp.zeros((tok_dev, slots), jnp.float32)
    for k in range(ids_ref.shape[1]):
        queue = slots_ref[:, k : k + 1]
        cell = jnp.where(queue < capacity, ids_ref[:, k : k + 1] * capacity + queue, slots)
        hit = grid == cell
        mix += jnp.where(hit, gates_ref[:, k : k + 1], 0.0)
        named += jnp.where(hit, 1.0, 0.0)
    mixing[...] = mix
    spread = named.T.astype(jnp.bfloat16)

    def fill(i, carry):
        cols = pl.ds(pl.multiple_of(i * step, step), step)
        rows = jnp.dot(spread, tokens_ref[:, cols], preferred_element_type=jnp.float32)
        outgoing[:, cols] = rows.astype(jnp.bfloat16)
        return carry

    lax.fori_loop(0, width // step, fill, 0)

    def rows_of(owner):
        return pl.ds(pl.multiple_of(owner * capacity, capacity), capacity)

    mine = rows_of(e)
    dispatched = [
        tracked(outgoing.at[rows_of(peer), :], incoming.at[mine, :], {"expert": peer})
        for peer in peers
    ]
    kept = local(outgoing.at[mine, :], incoming.at[mine, :])

    low, high = pl.ds(0, half_units), pl.ds(half_units, half_units)
    gate_y.wait_recv()
    gate_d0 = tracked(gate_buf.at[2, low, :], gate_buf.at[3, low, :], to_x)
    gate_x.wait_recv()
    gate_d1 = tracked(gate_buf.at[1, high, :], gate_buf.at[3, high, :], to_y)
    up_y.wait_recv()
    up_d0 = tracked(up_buf.at[2, low, :], up_buf.at[3, low, :], to_x)
    up_x.wait_recv()
    up_d1 = tracked(up_buf.at[1, high, :], up_buf.at[3, high, :], to_y)

    def down_own(c):
        cols = pl.ds(c * chunk, chunk)
        return (
            tracked(down_ref.at[0, :, cols], down_buf.at[1, :, cols], to_x),
            tracked(down_ref.at[0, :, cols], down_buf.at[2, :, cols], to_y),
        )

    def key_rows_at(owner, p, start=0, size=piece):
        first = (owner % 2) * key_half + p * piece + start
        return pl.ds(pl.multiple_of(first, half_piece), size)

    def key_own(p):
        rows = key_rows_at(e, p)
        return (
            tracked(key_ref.at[rows, :], key_buf.at[d, rows, :], to_x),
            tracked(key_ref.at[rows, :], key_buf.at[d, rows, :], to_y),
        )

    key_first, key_second, key_shared = [], [], []

    def pass_key(owner, rows, where):
        part = key_buf.at[owner, rows, :]
        return tracked(part, part, where)

    def key_share(owner, rows):
        key_shared.append(pass_key(owner, rows, to_sibling))

    def key_middle(p):
        key_x, key_y = key_first[p]
        rows = key_rows_at(e, p)
        key_y.wait_recv()
        d0 = pass_key(dy, key_rows_at(e, p, 0, half_piece), to_x)
        key_x.wait_recv()
        d1 = pass_key(dx, key_rows_at(e, p, half_piece, half_piece), to_y)
        key_second.append((d0, d1))
        key_share(dy, rows)
        key_share(dx, rows)

    def key_diagonal(p):
        d0, d1 = key_second[p]
        d0.wait_recv()
        key_share(dd, key_rows_at(e, p, 0, half_piece))
        d1.wait_recv()
        key_share(dd, key_rows_at(e, p, half_piece, half_piece))

    downs = [down_own(0), down_own(1)]

    for copy in dispatched:
        copy.wait_recv()
    kept.wait()
    own_gate.wait()
    own_up.wait()
    dims = (((1,), (1,)), ((), ()))

    def activate_slot(slot):
        acc_gate[...] = jnp.zeros_like(acc_gate)
        acc_up[...] = jnp.zeros_like(acc_up)

        def add(i, carry):
            cols = pl.ds(pl.multiple_of(i * step, step), step)
            rows = incoming[:, cols]
            acc_gate[...] += lax.dot_general(
                rows, gate_buf[slot, :, cols], dims, preferred_element_type=jnp.float32
            )
            acc_up[...] += lax.dot_general(
                rows, up_buf[slot, :, cols], dims, preferred_element_type=jnp.float32
            )
            return carry

        lax.fori_loop(0, width // step, add, 0)
        gate_act = acc_gate[...]
        hidden[slot] = (gate_act / (1.0 + jnp.exp(-gate_act)) * acc_up[...]).astype(jnp.bfloat16)

    def activate_loop(slot, carry):
        activate_slot(slot)
        return carry

    lax.fori_loop(0, 3, activate_loop, 0)
    for copy in (gate_d0, gate_d1, up_d0, up_d1):
        copy.wait_recv()
    activate_slot(3)
    own_down.wait()

    narrow = 256
    hands = []
    tile_first, tile_second = [], []
    acc_keys[...] = jnp.zeros_like(acc_keys)
    squares[...] = jnp.zeros_like(squares)

    def flag(owner, shard):
        return jnp.where(shard_ref[owner, 0] == shard, 1.0, 0.0)

    def ways(c):
        return (dx, dy, to_x, to_y) if c % 2 == 0 else (dy, dx, to_y, to_x)

    def combine(c):
        back, own = hands[c]
        for copy in back:
            copy.wait_recv()
        own.wait()
        mix = mixing[...]
        mix_hi = mix.astype(jnp.bfloat16)
        mix_lo = (mix - mix_hi.astype(jnp.float32)).astype(jnp.bfloat16)

        def blend(i, carry):
            at = pl.ds(pl.multiple_of(c * chunk + i * narrow, narrow), narrow)
            rows = returned[:, at]
            branch = jnp.dot(mix_hi, rows, preferred_element_type=jnp.float32)
            branch += jnp.dot(mix_lo, rows, preferred_element_type=jnp.float32)
            tiles[0, :, at] = (tokens_ref[:, at].astype(jnp.float32) + branch).astype(jnp.bfloat16)
            return carry

        lax.fori_loop(0, chunk // narrow, blend, 0)
        cols = pl.ds(c * chunk, chunk)
        tile_first.append(tracked(tiles.at[0, :, cols], tiles.at[1, :, cols], ways(c)[2]))

    def swap(c):
        near, far, _, to_far = ways(c)
        own = flag(d, far)
        tile_first[c].wait_recv()

        def mask(i, carry):
            at = pl.ds(pl.multiple_of(c * chunk + i * narrow, narrow), narrow)
            rows = own * tiles[0, :, at].astype(jnp.float32)
            rows += (1.0 - own) * tiles[1, :, at].astype(jnp.float32)
            passed[:, at] = rows.astype(jnp.bfloat16)
            return carry

        lax.fori_loop(0, chunk // narrow, mask, 0)
        cols = pl.ds(c * chunk, chunk)
        tile_second.append(tracked(passed.at[:, cols], tiles.at[2, :, cols], to_far))

    def finish(c):
        near = ways(c)[0]
        weights = [flag(d, d), flag(near, d)]
        weights.append(1.0 - weights[0] - weights[1])
        tile_second[c].wait_recv()

        def choose(i, carry):
            at = pl.ds(pl.multiple_of(c * chunk + i * narrow, narrow), narrow)
            rows = weights[0] * tiles[0, :, at].astype(jnp.float32)
            for slot in (1, 2):
                rows += weights[slot] * tiles[slot, :, at].astype(jnp.float32)
            student_ref[:, at] = rows.astype(jnp.bfloat16)
            gained[:, at] = (rows * gain_ref[:, at]).astype(jnp.bfloat16)
            squares[...] += jnp.sum(rows * rows, axis=-1, keepdims=True)
            return carry

        lax.fori_loop(0, chunk // narrow, choose, 0)

    def project_keys(c, carry):
        at = pl.ds(pl.multiple_of(c * chunk, chunk), chunk)
        per_owner = key_rows // chunk
        rows = pl.ds(pl.multiple_of((c % per_owner) * chunk, chunk), chunk)
        acc_keys[...] += jnp.dot(
            gained[:, at], key_buf[c // per_owner, rows, :], preferred_element_type=jnp.float32
        )
        return carry

    def follow(c):
        if 0 <= c - LAG < CHUNKS:
            combine(c - LAG)
        if 0 <= c - LAG - 1 < CHUNKS:
            swap(c - LAG - 1)
        if 0 <= c - LAG - 2 < CHUNKS:
            finish(c - LAG - 2)

    for c in range(CHUNKS):
        cols = pl.ds(c * chunk, chunk)
        down_x, down_y = downs[c]
        down_y.wait_recv()
        d0 = tracked(down_buf.at[2, low, cols], down_buf.at[3, low, cols], to_x)
        down_x.wait_recv()
        d1 = tracked(down_buf.at[1, high, cols], down_buf.at[3, high, cols], to_y)
        if c + 2 < CHUNKS:
            downs.append(down_own(c + 2))
        elif c + 1 == CHUNKS:
            key_first.extend(key_own(p) for p in range(PIECES))
        d0.wait_recv()
        d1.wait_recv()

        def project(i, carry):
            at = pl.ds(pl.multiple_of(c * chunk + i * narrow, narrow), narrow)
            total = jnp.dot(hidden[0], down_buf[0, :, at], preferred_element_type=jnp.float32)
            for slot in range(1, 4):
                total += jnp.dot(
                    hidden[slot], down_buf[slot, :, at], preferred_element_type=jnp.float32
                )
            produced[:, at] = total.astype(jnp.bfloat16)
            return carry

        lax.fori_loop(0, chunk // narrow, project, 0)
        back = [
            tracked(produced.at[rows_of(peer), cols], returned.at[mine, cols], {"expert": peer})
            for peer in peers
        ]
        hands.append((back, local(produced.at[mine, cols], returned.at[mine, cols])))

        follow(c)

    follow(CHUNKS)
    for p in range(PIECES):
        key_middle(p)
    follow(CHUNKS + 1)
    for p in range(PIECES):
        key_diagonal(p)
    own_key.wait()
    for copy in key_shared:
        copy.wait_recv()
    ready = CHUNKS + 2 - LAG - 2
    lax.fori_loop(0, ready, project_keys, 0)
    for c in range(CHUNKS + 2, CHUNKS + LAG + 2):
        follow(c)
        project_keys(c - LAG - 2, 0)
    scale = lax.rsqrt(squares[...] / width + 1e-05)
    keys_ref[...] = (acc_keys[...] * scale).astype(jnp.bfloat16)
    for copy in sent:
        copy.wait_send()


def fused(
    tokens,
    gate_proj,
    up_proj,
    down_proj,
    route_ids,
    route_slots,
    route_gates,
    image_shard,
    norm_gain,
    key_proj,
    capacity,
):
    tok_dev, width = tokens.shape
    n_expert = lax.axis_size("expert")
    slots = n_expert * capacity
    units = gate_proj.shape[1]
    key_rows, key_width = key_proj.shape
    remote = 8 + 8 * PIECES + (n_expert - 1) * (1 + CHUNKS) + 6 * CHUNKS
    vmem = pl.BlockSpec(memory_space=pltpu.VMEM)
    anywhere = pl.BlockSpec(memory_space=pl.ANY)
    scalars = pl.BlockSpec(memory_space=pltpu.SMEM)
    half = jnp.bfloat16
    return pl.pallas_call(
        functools.partial(fused_kernel, n_expert, capacity),
        out_shape=(
            jax.ShapeDtypeStruct((tok_dev, width), half),
            jax.ShapeDtypeStruct((tok_dev, key_width), half),
        ),
        in_specs=[vmem] * 3 + [scalars] + [vmem] * 2 + [anywhere] * 4,
        out_specs=(vmem, vmem),
        scratch_shapes=[
            pltpu.VMEM((4, units, width), half),
            pltpu.VMEM((4, units, width), half),
            pltpu.VMEM((4, units, width), half),
            pltpu.VMEM((4, key_rows, key_width), half),
            pltpu.VMEM((slots, width), half),
            pltpu.VMEM((slots, width), half),
            pltpu.VMEM((slots, width), half),
            pltpu.VMEM((slots, width), half),
            pltpu.VMEM((3, tok_dev, width), half),
            pltpu.VMEM((tok_dev, width), half),
            pltpu.VMEM((4, slots, units), half),
            pltpu.VMEM((tok_dev, width), half),
            pltpu.VMEM((tok_dev, slots), jnp.float32),
            pltpu.VMEM((tok_dev, key_width), jnp.float32),
            pltpu.VMEM((slots, units), jnp.float32),
            pltpu.VMEM((slots, units), jnp.float32),
            pltpu.VMEM((tok_dev, 1), jnp.float32),
            pltpu.SemaphoreType.DMA((remote,)),
            pltpu.SemaphoreType.DMA((remote,)),
            pltpu.SemaphoreType.DMA((5 + CHUNKS,)),
        ],
        compiler_params=pltpu.CompilerParams(
            collective_id=0, has_side_effects=True, vmem_limit_bytes=60 * 1024 * 1024
        ),
    )(
        route_ids,
        route_slots,
        route_gates,
        image_shard,
        norm_gain.reshape(1, -1),
        tokens,
        gate_proj,
        up_proj,
        down_proj,
        key_proj,
    )


def per_device(
    tokens,
    gate_proj,
    up_proj,
    down_proj,
    route_ids,
    route_slots,
    route_gates,
    image_shard,
    norm_gain,
    key_proj,
):
    tok_dev, model_width = tokens.shape
    top_count = route_ids.shape[1]
    experts = gate_proj.shape[0] * lax.axis_size("expert")
    capacity = 3 * tok_dev * top_count // (2 * experts)
    if capacity % 16 == 0 and gate_proj.shape[0] == 1 and lax.axis_size("dp") == 4 and experts % 2 == 0:
        if tok_dev == IMG_TOK and gate_proj.shape[1] % 32 == 0 and key_proj.shape[0] % 512 == 0:
            return fused(
                tokens,
                gate_proj,
                up_proj,
                down_proj,
                route_ids,
                route_slots,
                route_gates,
                image_shard,
                norm_gain,
                key_proj,
                capacity,
            )
    slot_total = experts * capacity
    retained = route_slots < capacity
    slot_cells = jnp.where(retained, route_ids * capacity + route_slots, slot_total).reshape(-1)
    owners = jnp.arange(tok_dev * top_count, dtype=jnp.int32) // top_count
    cell_token = (
        jnp.full((slot_total + 1,), tok_dev, jnp.int32).at[slot_cells].set(owners)[:slot_total]
    )
    outgoing = jnp.take(tokens, cell_token, axis=0, mode="fill", fill_value=0).reshape(
        experts, capacity, model_width
    )
    arrived = lax.all_to_all(outgoing, "expert", split_axis=0, concat_axis=0, tiled=True)
    incoming = arrived.reshape(-1, model_width)
    hidden = activate(
        incoming,
        lax.all_gather(gate_proj, "dp", axis=1, tiled=True)[0],
        lax.all_gather(up_proj, "dp", axis=1, tiled=True)[0],
    )
    summed = jnp.dot(
        hidden,
        lax.all_gather(down_proj, "dp", axis=1, tiled=True)[0],
        preferred_element_type=jnp.float32,
    )
    produced = summed.astype(jnp.bfloat16).reshape(arrived.shape)
    returned = lax.all_to_all(produced, "expert", split_axis=0, concat_axis=0, tiled=True).reshape(
        -1, model_width
    )
    picked = jnp.take(returned, slot_cells, axis=0, mode="fill", fill_value=0).reshape(
        tok_dev, top_count, model_width
    )
    mixing = jnp.where(retained, route_gates, 0.0)
    branch = jnp.einsum("tk,tkd->td", mixing, picked.astype(jnp.float32))
    teacher = (tokens.astype(jnp.float32) + branch).astype(jnp.bfloat16)
    gathered = lax.all_gather(teacher, "dp", axis=0, tiled=True)
    shard_column = image_shard.reshape(-1)
    images_col = shard_column.shape[0]
    arrangement = jnp.argsort(shard_column * images_col + jnp.arange(images_col, dtype=jnp.int32))
    images = gathered.reshape(images_col, IMG_TOK, model_width)
    position = lax.axis_index("dp")
    ordered = jnp.take(images, arrangement, axis=0).reshape(images_col * IMG_TOK, model_width)
    student_rows = lax.dynamic_slice_in_dim(ordered, position * tok_dev, tok_dev, 0)
    normed = normalize(ordered, norm_gain)
    columns = lax.dynamic_slice_in_dim(normed, position * key_proj.shape[0], key_proj.shape[0], 1)
    projected = lax.psum_scatter(
        jnp.dot(columns, key_proj, preferred_element_type=jnp.float32),
        "dp",
        scatter_dimension=0,
        tiled=True,
    )
    return (student_rows, projected.astype(jnp.bfloat16))


def solution(mesh):
    in_specs = (
        P(("dp", "expert"), None),
        P("expert", "dp", None),
        P("expert", "dp", None),
        P("expert", "dp", None),
        P(("dp", "expert"), None),
        P(("dp", "expert"), None),
        P(("dp", "expert"), None),
        P(None, "expert"),
        P(),
        P("dp", None),
    )
    out_specs = (P(("dp", "expert"), None), P(("dp", "expert"), None))
    return jax.shard_map(
        per_device, mesh=mesh, in_specs=in_specs, out_specs=out_specs, check_vma=False
    )
```
